32 devices in a mesh: chip: 2 (over y), board: 4 (over z), cuts: 4 (over x, core).
Axes of the slice: x: 2, y: 2, z: 4, core: 2. Of those that a mesh axis runs over, the one named last changes fastest.
Arguments:
- features: bfloat16 [32, 2048, 1024], P(('chip', 'board', 'cuts')), may hold values from -6 to 6
- targets: bfloat16 [32, 2048, 256], P(('chip', 'board', 'cuts')), may hold values from -24 to 24
- lower_weight: bfloat16 [32, 1024, 512], P(('chip', 'board', 'cuts')), may hold values from -0.1875 to 0.1875
- head_weight: float32 [32, 512, 256], P(('chip', 'board', 'cuts')), may hold values from -0.25 to 0.25
- batch_rows: int32 [32, 2, 1024], P(('chip', 'board', 'cuts')), may hold values from 0 to 2047
- sample_counts: int32 [32], P(('chip', 'board', 'cuts')), may hold values from 1 to 1000
- cluster_ids: int32 [32], P(('chip', 'board', 'cuts')), may hold values from 0 to 7, as said below
Outputs:
- cluster_step: float32 [32, 512, 256], P(('chip', 'board', 'cuts'))
The draws below stay inside these ranges and needn't reach their ends.
Inputs may be any that keep to these rules, and one draw needn't show every extreme that they name: `cluster_ids`: every one of the 8 clusters has at least one client.
All inputs are finite; a program needn't handle non-finite values.
Results may differ from the reference program's by a relative error of at most 0.0003.
Values sent between devices are 32-bit elements; how exact they have to be, the bound alone decides.
A program may use at most 64 MiB of HBM per device.

```python
import jax
import jax.numpy as jnp
from jax import lax

IN = 1024
HID = 512
OUT = 256
CLUSTERS = 8
STEPS = 2
POOL = 2048
ROWS = 1024
CLIENTS = 32


def draw_cluster_ids(key, part):
    first = jax.random.fold_in(key, 11)
    second = jax.random.fold_in(key, 23)
    drawn = jax.random.randint(first, (CLIENTS,), 0, CLUSTERS, dtype=jnp.int32)
    order = jax.random.permutation(second, CLIENTS)
    return drawn.at[order[:CLUSTERS]].set(jnp.arange(CLUSTERS, dtype=jnp.int32))


def with_ends(values, rng, smallest, largest):
    index_at = [jax.random.randint(jax.random.fold_in(rng, axis), (), 0, length) for axis, length in enumerate(values.shape)]
    widest = values.shape.index(max(values.shape))
    neighbour = index_at[:widest] + [(index_at[widest] + 1) % values.shape[widest]] + index_at[widest + 1:]
    return values.at[tuple(index_at)].set(smallest).at[tuple(neighbour)].set(largest)


def level_of(key, shape, cuts, low, largest):
    def one(dim, parts):
        draws = jax.random.uniform(jax.random.fold_in(jax.random.fold_in(key, 6), dim), (parts,), jnp.float32, low / len(cuts), largest / len(cuts))
        return jnp.repeat(jnp.exp(draws), shape[dim] // parts).reshape((-1,) + (1,) * (len(shape) - dim - 1))

    gain = one(*cuts[0])
    for cut in cuts[1:]:
        gain = gain * one(*cut)
    return gain


def centred(key, shape, width, limit, cuts=(), kind=jnp.bfloat16):
    result = jax.random.normal(key, shape, jnp.float32) * width
    if len(cuts) > 0:
        result = level_of(key, shape, cuts, -0.22, 0.18) * result
    return jnp.clip(result, min=-limit, max=limit).astype(kind)


def setup_inputs(seed: int = 0) -> dict:
    arg_keys = jax.random.split(jax.random.key(seed), 8)
    return {
        "features": centred(arg_keys[0], (CLIENTS, POOL, IN), 1.0, 6.0, ((0, 32),)),
        "targets": centred(arg_keys[1], (CLIENTS, POOL, OUT), 4.0, 24.0, ((0, 32),)),
        "lower_weight": centred(arg_keys[2], (CLIENTS, IN, HID), IN ** -0.5, 0.1875, ((0, 32),)),
        "head_weight": centred(arg_keys[3], (CLIENTS, HID, OUT), HID ** -0.5, 0.25, ((0, 32),), jnp.float32),
        "batch_rows": with_ends(jax.random.randint(arg_keys[4], (CLIENTS, STEPS, ROWS), 0, POOL), jax.random.fold_in(arg_keys[4], 1), 0, POOL - 1).astype(jnp.int32),
        "sample_counts": with_ends(jax.random.randint(arg_keys[5], (CLIENTS,), 1, 1001), jax.random.fold_in(arg_keys[5], 1), 1, 1000).astype(jnp.int32),
        "cluster_ids": draw_cluster_ids(jax.random.fold_in(arg_keys[7], 71), 0),
    }


LR = 0.5


def one_client(args):
    feats, targs, lower, head, rows = args
    hidden = jnp.tanh(jnp.dot(feats, lower, preferred_element_type=jnp.float32))
    weight = head
    for step in range(STEPS):
        picked = jnp.take(hidden, rows[step], axis=0)
        wanted = jnp.take(targs, rows[step], axis=0).astype(jnp.float32)
        err = jnp.dot(picked, weight, precision=lax.Precision.HIGHEST) - wanted
        grad = jnp.dot(picked.T, err, precision=lax.Precision.HIGHEST) / ROWS
        weight = weight - LR * grad
    return weight - head


def reference(features, targets, lower_weight, head_weight, batch_rows, sample_counts, cluster_ids):
    deltas = lax.map(one_client, (features, targets, lower_weight, head_weight, batch_rows))
    onehot = (cluster_ids[:, None] == jnp.arange(CLUSTERS, dtype=jnp.int32)[None, :]).astype(jnp.float32)
    weighted = onehot * sample_counts.astype(jnp.float32)[:, None]
    flat = deltas.reshape(CLIENTS, HID * OUT)
    sums = jnp.dot(weighted.T, flat, precision=lax.Precision.HIGHEST)
    counts = jnp.sum(weighted, axis=0)
    mine = jnp.take(sums, cluster_ids, axis=0).reshape(CLIENTS, HID, OUT)
    denom = jnp.take(counts, cluster_ids, axis=0)
    return mine / (LR * denom)[:, None, None]
```

```python
import functools

import jax
import jax.numpy as jnp
from jax import lax
from jax.experimental import pallas as pl
from jax.experimental.pallas import tpu as pltpu
from jax.sharding import PartitionSpec as P

LR = 0.5
CLUSTERS = 8
LANES = 128
TILE = 256
CHUNKS = 8
LAG = 2
MESH = pl.DeviceIdType.MESH


def halves(value):
    high = value.astype(jnp.bfloat16)
    low = (value - high.astype(jnp.float32)).astype(jnp.bfloat16)
    return high, low


def dot(a, b):
    return jnp.dot(a, b, preferred_element_type=jnp.float32)


def dot_rows(a, b):
    return lax.dot_general(a, b, (((0,), (0,)), ((), ())), preferred_element_type=jnp.float32)


def local_kernel(x_hbm, lower_ref, target_ref, head_ref, rows_ref, delta_ref, x_buf, hid_hi, hid_lo, drawn, w_hi, w_lo, x_sem):
    pool = x_buf.shape[0]
    tile = min(TILE, pool)
    tiles = pool // tile
    steps, count_rows = rows_ref.shape[1], rows_ref.shape[2]
    width = head_ref.shape[2]

    def x_copy(i):
        part = pl.ds(pl.multiple_of(i * tile, tile), tile)
        return pltpu.make_async_copy(x_hbm.at[0, part], x_buf.at[part], x_sem.at[i])

    for i in range(tiles):
        x_copy(i).start()

    blocks = pool // LANES
    for step in range(steps):
        rows = rows_ref[0, step : step + 1, :]
        outer = lax.shift_right_logical(rows, 7)
        inner = lax.bitwise_and(rows, LANES - 1)
        one_outer = (lax.broadcasted_iota(jnp.int32, (blocks, count_rows), 0) == outer).astype(jnp.float32).astype(jnp.bfloat16)
        one_inner = (lax.broadcasted_iota(jnp.int32, (LANES, count_rows), 0) == inner).astype(jnp.float32).astype(jnp.bfloat16)
        table = lax.dot_general(one_inner, one_outer, (((1,), (1,)), ((), ())), preferred_element_type=jnp.float32)
        for j in range(blocks):
            drawn[step, j * LANES : (j + 1) * LANES, :] = jnp.broadcast_to(table[:, j : j + 1], (LANES, LANES))

    high, low = halves(head_ref[0])
    w_hi[...] = high
    w_lo[...] = low
    delta_ref[...] = jnp.zeros_like(delta_ref)
    scale = -LR / count_rows

    for step in range(steps):

        @pl.loop(0, tiles)
        def _(i):
            part = pl.ds(pl.multiple_of(i * tile, tile), tile)
            if step == 0:
                x_copy(i).wait()
                hidden = jnp.tanh(dot(x_buf[part, :], lower_ref[0]))
                h_hi, h_lo = halves(hidden)
                hid_hi[part, :] = h_hi
                hid_lo[part, :] = h_lo
            else:
                h_hi = hid_hi[part, :]
                h_lo = hid_lo[part, :]
            err = dot(h_hi, w_hi[...]) + dot(h_hi, w_lo[...]) + dot(h_lo, w_hi[...])
            err = err - target_ref[0, part, :].astype(jnp.float32)
            times = drawn[step, part, :]
            err = err * jnp.concatenate([times] * (width // LANES), axis=1) * scale
            e_hi, e_lo = halves(err)
            delta_ref[...] += dot_rows(h_hi, e_hi) + dot_rows(h_hi, e_lo) + dot_rows(h_lo, e_hi)

        if step + 1 < steps:
            high, low = halves(head_ref[0] + delta_ref[...])
            w_hi[...] = high
            w_lo[...] = low


def local_delta(features, targets, lower_weight, head_weight, batch_rows):
    pool, features_in = features.shape[1:]
    hid, out = head_weight.shape[1:]
    vmem = pl.BlockSpec(memory_space=pltpu.VMEM)
    tiles = pool // min(TILE, pool)
    return pl.pallas_call(
        local_kernel,
        name="local_steps",
        out_shape=jax.ShapeDtypeStruct((hid, out), jnp.float32),
        in_specs=[pl.BlockSpec(memory_space=pl.ANY), vmem, vmem, vmem, vmem],
        out_specs=vmem,
        scratch_shapes=[
            pltpu.VMEM((pool, features_in), jnp.bfloat16),
            pltpu.VMEM((pool, hid), jnp.bfloat16),
            pltpu.VMEM((pool, hid), jnp.bfloat16),
            pltpu.VMEM((batch_rows.shape[1], pool, LANES), jnp.float32),
            pltpu.VMEM((hid, out), jnp.bfloat16),
            pltpu.VMEM((hid, out), jnp.bfloat16),
            pltpu.SemaphoreType.DMA((tiles,)),
        ],
        compiler_params=pltpu.CompilerParams(vmem_limit_bytes=40 * 2**20),
    )(features, lower_weight, targets, head_weight, batch_rows)


def mean_kernel(
    sizes, chunks, id_ref, count_ref, delta_ref, out_ref,
    facts, chosen, inbox, own, from_left, from_right, to_right, to_left, outbox, result,
    fact_send, fact_recv, share_send, share_recv, right_send, right_recv, left_send, left_recv, back_send, back_recv,
):
    chip_count, board_count, cuts_count = sizes
    plane = chip_count * cuts_count
    number = plane * board_count
    chip, board, cuts = lax.axis_index("chip"), lax.axis_index("board"), lax.axis_index("cuts")
    seat = chip * cuts_count + cuts
    me = board * plane + seat
    hid, width = delta_ref.shape
    block = hid // chunks
    share = block // plane

    def at(board_index, seat_index):
        return (seat_index // cuts_count, board_index, lax.rem(seat_index, cuts_count))

    def rows_of(k, seat_index):
        return pl.ds(pl.multiple_of(k * block + seat_index * share, 8), share)

    barrier = pltpu.get_barrier_semaphore()

    def greet(offset, carry):
        other = lax.rem(me + offset, number)
        pl.semaphore_signal(barrier, inc=1, device_id=at(other // plane, lax.rem(other, plane)), device_id_type=MESH)
        return carry

    lax.fori_loop(1, number, greet, 0)
    kind = lax.broadcasted_iota(jnp.int32, (CLUSTERS, LANES), 0)
    facts[me] = jnp.where(kind == id_ref[0], count_ref[0].astype(jnp.float32), 0.0)
    pl.semaphore_wait(barrier, number - 1)

    def tell(offset, carry):
        other = lax.rem(me + offset, number)
        pltpu.make_async_remote_copy(
            src_ref=facts.at[me], dst_ref=facts.at[me], send_sem=fact_send, recv_sem=fact_recv,
            device_id=at(other // plane, lax.rem(other, plane)), device_id_type=MESH,
        ).start()
        return carry

    lax.fori_loop(1, number, tell, 0)

    for k in range(chunks):

        def give(offset, carry, k=k):
            other = lax.rem(seat + offset, plane)
            pltpu.make_async_remote_copy(
                src_ref=delta_ref.at[rows_of(k, other)], dst_ref=inbox.at[k, seat],
                send_sem=share_send, recv_sem=share_recv.at[k],
                device_id=at(board, other), device_id_type=MESH,
            ).start()
            return carry

        lax.fori_loop(1, plane, give, 0)
        inbox[k, seat] = delta_ref[rows_of(k, seat), :]

    def arrived(ref, sem):
        pltpu.make_async_copy(ref, ref, sem).wait()

    arrived(facts.at[pl.ds(0, number - 1)], fact_recv)
    counts = jnp.sum(facts[...], axis=0)
    inverse = 1.0 / (LR * jnp.maximum(counts, 1.0))
    for t in range(plane):
        chosen[t] = jnp.where(facts[board * plane + t] > 0, inverse, 0.0)

    def wide(row):
        return jnp.concatenate([row] * (width // LANES), axis=1)

    def right_copy(k):
        return pltpu.make_async_remote_copy(
            src_ref=to_right.at[k], dst_ref=from_left.at[k], send_sem=right_send.at[k], recv_sem=right_recv.at[k],
            device_id=at(board + 1, seat), device_id_type=MESH,
        )

    def left_copy(k):
        return pltpu.make_async_remote_copy(
            src_ref=to_left.at[k], dst_ref=from_right.at[k], send_sem=left_send.at[k], recv_sem=left_recv.at[k],
            device_id=at(board - 1, seat), device_id_type=MESH,
        )

    last = board_count - 1

    def add_up(k):
        arrived(inbox.at[k, pl.ds(0, plane - 1)], share_recv.at[k])
        sums = [jnp.zeros((share, width), jnp.float32)] * CLUSTERS
        for t in range(plane):
            value = inbox[k, t]
            for c in range(CLUSTERS):
                sums[c] = sums[c] + wide(facts[board * plane + t, c : c + 1, :]) * value
        for c in range(CLUSTERS):
            own[k, c] = sums[c]

    def pass_right(k):
        @pl.when(board == 0)
        def _():
            from_left[k] = jnp.zeros_like(from_left[k])

        @pl.when(board > 0)
        def _():
            arrived(from_left.at[k], right_recv.at[k])

        @pl.when(board < last)
        def _():
            to_right[k] = own[k] + from_left[k]
            right_copy(k).start()

    def pass_left(k):
        @pl.when(board == last)
        def _():
            from_right[k] = jnp.zeros_like(from_right[k])

        @pl.when(board < last)
        def _():
            arrived(from_right.at[k], left_recv.at[k])

        @pl.when(board > 0)
        def _():
            to_left[k] = own[k] + from_right[k]
            left_copy(k).start()

    def give_back(k):
        total = [own[k, c] + from_left[k, c] + from_right[k, c] for c in range(CLUSTERS)]
        for t in range(plane):
            value = wide(chosen[t, 0:1, :]) * total[0]
            for c in range(1, CLUSTERS):
                value = value + wide(chosen[t, c : c + 1, :]) * total[c]
            outbox[k, t] = value
        result[rows_of(k, seat), :] = outbox[k, seat]

        def give(offset, carry):
            other = lax.rem(seat + offset, plane)
            pltpu.make_async_remote_copy(
                src_ref=outbox.at[k, other], dst_ref=result.at[rows_of(k, seat)],
                send_sem=back_send, recv_sem=back_recv,
                device_id=at(board, other), device_id_type=MESH,
            ).start()
            return carry

        lax.fori_loop(1, plane, give, 0)

    right_lag = LAG * board
    left_lag = LAG * (last - board)
    back_lag = jnp.maximum(right_lag, left_lag)

    def tick(step, carry):
        for lag, act in ((0, add_up), (right_lag, pass_right), (left_lag, pass_left), (back_lag, give_back)):
            k = step - lag

            @pl.when((k >= 0) & (k < chunks))
            def _():
                act(k)

        return carry

    lax.fori_loop(0, chunks + LAG * last, tick, 0)

    moved = pl.ds(0, chunks * (plane - 1) * share)
    arrived(result.at[moved], back_recv)
    out_ref[0] = result[...]
    arrived(result.at[moved], back_send)
    arrived(result.at[moved], share_send)
    arrived(facts.at[pl.ds(0, number - 1)], fact_send)

    @pl.when(board < last)
    def _():
        for k in range(chunks):
            arrived(to_right.at[k], right_send.at[k])

    @pl.when(board > 0)
    def _():
        for k in range(chunks):
            arrived(to_left.at[k], left_send.at[k])


def cluster_mean(sizes, delta, sample_counts, cluster_ids):
    hid, width = delta.shape
    plane = sizes[0] * sizes[2]
    number = plane * sizes[1]
    chunks = max(1, min(CHUNKS, hid // (plane * 8)))
    share = hid // (chunks * plane)
    vmem = pl.BlockSpec(memory_space=pltpu.VMEM)
    smem = pl.BlockSpec(memory_space=pltpu.SMEM)
    sums = pltpu.VMEM((chunks, CLUSTERS, share, width), jnp.float32)
    shares = pltpu.VMEM((chunks, plane, share, width), jnp.float32)
    one, many = pltpu.SemaphoreType.DMA, pltpu.SemaphoreType.DMA((chunks,))
    return pl.pallas_call(
        functools.partial(mean_kernel, sizes, chunks),
        name="cluster_mean",
        out_shape=jax.ShapeDtypeStruct((1, hid, width), jnp.float32),
        in_specs=[smem, smem, vmem],
        out_specs=vmem,
        scratch_shapes=[
            pltpu.VMEM((number, CLUSTERS, LANES), jnp.float32),
            pltpu.VMEM((plane, CLUSTERS, LANES), jnp.float32),
            shares, sums, sums, sums, sums, sums, shares,
            pltpu.VMEM((hid, width), jnp.float32),
            one, one, one, many, many, many, many, many, one, one,
        ],
        compiler_params=pltpu.CompilerParams(collective_id=0, has_side_effects=True, vmem_limit_bytes=40 * 2**20),
    )(cluster_ids, sample_counts, delta)


def solution(mesh):
    sizes = (mesh.shape["chip"], mesh.shape["board"], mesh.shape["cuts"])

    def on_device(features, targets, lower_weight, head_weight, batch_rows, sample_counts, cluster_ids):
        delta = local_delta(features, targets, lower_weight, head_weight, batch_rows)
        return cluster_mean(sizes, delta, sample_counts, cluster_ids)

    rows, flat = P(("chip", "board", "cuts"), None, None), P(("chip", "board", "cuts"))
    return jax.shard_map(
        on_device,
        mesh=mesh,
        in_specs=(rows, rows, rows, rows, rows, flat, flat),
        out_specs=rows,
        check_vma=False,
    )
```
